1024 devices in a mesh: dp: 4 (over y), expert: 64 (over z, core), tensor: 4 (over x).
Axes of the slice: x: 4, y: 4, z: 32, core: 2. Of those that a mesh axis runs over, the one named last changes fastest.
Arguments:
- tokens: bfloat16 [1536, 7168], P('expert', 'tensor'), may hold values from -6 to 6
- expert_ids: int32 [1536, 8], P('expert'), may hold values from 0 to 63, all different within a row; in each aligned block of 24 rows (0 to 23, 24 to 47, ...) at most 4 rows name the same one
- gate_weights: float32 [1536, 8], P('expert'), may hold values from 0.1 to 1
- w_gate: bfloat16 [64, 7168, 1024], P('expert', 'tensor', 'dp'), may hold values from -0.0625 to 0.0625
- w_up: bfloat16 [64, 7168, 1024], P('expert', 'tensor', 'dp'), may hold values from -0.0625 to 0.0625
- w_down: bfloat16 [64, 1024, 7168], P('expert', 'dp', 'tensor'), may hold values from -0.1875 to 0.1875
Outputs:
- mixed: bfloat16 [1536, 7168], P('expert', 'tensor')
The draws below stay inside these ranges and needn't reach their ends.
Inputs may be any that keep to these rules, and one draw needn't show every extreme that they name: `expert_ids`: each row names 8 different experts. Among the rows of one index of the expert axis (aligned blocks of 24 rows) no expert is named more than 4 times, and in some block one expert is named exactly 4 times.
All inputs are finite; a program needn't handle non-finite values.
Results may differ from the reference program's by a relative error of at most 0.0049.
Values may be sent and summed in bfloat16 or wider, within the bound.
A program may use at most 32 MiB of HBM per device.

```python
import math
import jax
import jax.numpy as jnp
import numpy as np
from jax import lax

D = 7168
FF = 1024
TOP = 8
EXPERTS = 64
T_DEV = 24
CAP = 4
TOKENS = 1536
N_EXPERT = 64


def level_of(rng, dims, cuts, smallest, high):
    def one(axis_at, blocks):
        heights = jax.random.uniform(jax.random.fold_in(jax.random.fold_in(rng, 6), axis_at), (blocks,), jnp.float32, smallest / len(cuts), high / len(cuts))
        return jnp.repeat(jnp.exp(heights), dims[axis_at] // blocks).reshape((-1,) + (1,) * (len(dims) - axis_at - 1))

    gain = one(*cuts[0])
    for cut in cuts[1:]:
        gain = gain * one(*cut)
    return gain


def shared_out(key, own, number, rows, count, top, bound, slope):
    ranking = jax.random.permutation(key, count)
    packed, ordinary = shares(count, rows * top, bound, slope, True), shares(count, rows * top, bound, slope, False)
    places = jnp.arange(count)

    def named(lengths, turn):
        used = int((lengths > 0).sum())
        fixed = max(1, used // 4)
        shifted = fixed + (places - fixed + turn * (used - fixed)) % max(1, count - fixed)
        return jnp.zeros((count,), jnp.int32).at[ranking[jnp.where(places < fixed, places, shifted)]].set(jnp.asarray(lengths, jnp.int32))

    lengths = jnp.where(number % 4 == 0, named(packed, number // 4), named(ordinary, number - number // 4 - 1))
    mixed = jax.random.permutation(jax.random.fold_in(own, 3), count)
    giver, taker = mixed[0:count // 2 * 2:2], mixed[1:count // 2 * 2:2]
    room = jnp.minimum(lengths[giver] - 1, bound - lengths[taker]) // 2
    room = jnp.where((giver == ranking[0]) | (taker == ranking[0]) | (lengths[taker] == 0), 0, jnp.maximum(room, 0))
    shifted = jax.random.randint(jax.random.fold_in(own, 4), (count // 2,), 0, 1 << 20) % (room + 1)
    lengths = lengths.at[giver].add(-shifted).at[taker].add(shifted)
    members = jnp.searchsorted(jnp.cumsum(lengths), jnp.arange(rows * top), side="right").astype(jnp.int32)
    table = members.reshape(top, rows).T
    table = table[jax.random.permutation(jax.random.fold_in(own, 1), rows)]
    turn = jax.random.randint(jax.random.fold_in(own, 2), (rows, 1), 0, top)
    return jnp.take_along_axis(table, (jnp.arange(top)[None, :] + turn) % top, axis=1)


def shares(count, total, most, skew, full):
    portions = [(1 << 20) // math.isqrt(standing ** skew) + 1 for standing in range(1, count + 1)]
    largest = most if full else min(most, max(-(-total // count), total * portions[0] // sum(portions)))
    least = 1 if total - largest >= count - 1 else 0
    given, spare = [largest] + [least] * (count - 1), total - largest - least * (count - 1)
    while spare > 0:
        candidates = [i for i in range(1, count) if given[i] < largest] or [i for i in range(1, count) if given[i] < most]
        mass, remaining = sum([portions[i] for i in candidates]), spare
        for i in candidates:
            addition = min(most - given[i], max(1, remaining * portions[i] // mass), spare)
            given[i] = given[i] + addition
            spare = spare - addition
    return np.array(given)


def noise(key, shape, deviation, most, shards=(), held_as=jnp.bfloat16):
    drawn = jax.random.normal(key, shape, jnp.float32) * deviation
    if len(shards) > 0:
        drawn = level_of(key, shape, shards, -0.22, 0.18) * drawn
    return jnp.clip(drawn, min=-most, max=most).astype(held_as)


def setup_inputs(seed: int = 0) -> dict:
    key_of = jax.random.split(jax.random.key(seed), 7)
    tokens = noise(key_of[0], (TOKENS, D), 1.0, 6.0, ((0, 64), (1, 4)))
    expert_ids_keys = jax.random.split(jax.random.fold_in(key_of[1], 1), TOKENS // T_DEV)
    expert_ids_turns = jax.random.permutation(jax.random.fold_in(key_of[1], 3), TOKENS // T_DEV)
    expert_ids = jax.vmap(lambda own, number: shared_out(jax.random.fold_in(key_of[1], 2), own, number, T_DEV, EXPERTS, TOP, CAP, 2))(expert_ids_keys, expert_ids_turns).reshape((TOKENS, TOP))
    gate_weights = jnp.clip(jnp.exp(math.log(1.0) - 2.3025851 * jax.random.uniform(key_of[2], (TOKENS, TOP), jnp.float32) ** level_of(key_of[2], (TOKENS, TOP), ((0, 64),), -0.2, 0.2)), 0.1, 1.0)
    w_gate = noise(key_of[3], (EXPERTS, D, FF), D ** -0.5, 0.0625, ((0, 64), (1, 4), (2, 4)))
    w_up = noise(key_of[4], (EXPERTS, D, FF), D ** -0.5, 0.0625, ((0, 64), (1, 4), (2, 4)))
    w_down = noise(key_of[5], (EXPERTS, FF, D), FF ** -0.5, 0.1875, ((0, 64), (1, 4), (2, 4)))
    return {"tokens": tokens, "expert_ids": expert_ids, "gate_weights": gate_weights, "w_gate": w_gate, "w_up": w_up, "w_down": w_down}


def reference(tokens, expert_ids, gate_weights, w_gate, w_up, w_down):
    assignments = TOKENS * TOP
    slots_per_expert = N_EXPERT * CAP
    flat_ids = expert_ids.reshape(-1).astype(jnp.int32)
    sort_order = jnp.argsort(flat_ids, stable=True).astype(jnp.int32)
    sorted_ids = flat_ids[sort_order]
    totals = jnp.sum((flat_ids[:, None] == jnp.arange(EXPERTS, dtype=jnp.int32)[None, :]).astype(jnp.int32), axis=0)
    offsets = (jnp.cumsum(totals) - totals).astype(jnp.int32)
    slot_rank = jnp.arange(assignments, dtype=jnp.int32) - offsets[sorted_ids]
    slot_table = jnp.full((EXPERTS * slots_per_expert,), assignments, jnp.int32)
    slot_table = slot_table.at[sorted_ids * slots_per_expert + slot_rank].set(sort_order)
    slot_table = slot_table.reshape(EXPERTS, slots_per_expert)
    padded_tokens = jnp.concatenate([tokens, jnp.zeros((1, D), tokens.dtype)], axis=0)
    padded_weights = jnp.concatenate([gate_weights.reshape(-1), jnp.zeros((1,), gate_weights.dtype)])

    def one_expert(running, inputs):
        entries, gate_matrix, up_matrix, down_matrix = inputs
        token_rows = (entries // TOP).astype(jnp.int32)
        chosen = padded_tokens[token_rows]
        gate_pre = jnp.dot(chosen, gate_matrix, preferred_element_type=jnp.float32)
        up_pre = jnp.dot(chosen, up_matrix, preferred_element_type=jnp.float32)
        hidden = (jax.nn.silu(gate_pre) * up_pre).astype(jnp.bfloat16)
        expert_out = jnp.dot(hidden, down_matrix, preferred_element_type=jnp.float32)
        running = running.at[token_rows].add(expert_out * padded_weights[entries][:, None])
        return running, None

    initial = jnp.zeros((TOKENS + 1, D), jnp.float32)
    running, _ = lax.scan(one_expert, initial, (slot_table, w_gate, w_up, w_down))
    return running[:TOKENS].astype(jnp.bfloat16)
```

```python
import jax
import jax.numpy as jnp
from jax import lax
from jax.sharding import Mesh
from jax.sharding import PartitionSpec as P

TOP = 8
CAP = 4
EXPERT = ("expert_0", "expert_1")


def cut_along(value, dim, size):
    shape = value.shape
    pieces = value.reshape(*shape[:dim], size, shape[dim] // size, *shape[dim + 1 :])
    return jnp.moveaxis(pieces, dim, 0)


def in_order(pieces, dim):
    shape = list(pieces.shape[1:])
    shape[dim] *= pieces.shape[0]
    return jnp.moveaxis(pieces, 0, dim).reshape(shape)


def moved_by_axis(pieces, axes, turns):
    inside = pieces.shape[1:]
    filled = pieces.reshape(*(lax.axis_size(a) for a in axes), *inside)
    for k in turns:
        filled = lax.all_to_all(filled, axes[k], k, k, tiled=True)
    return filled.reshape(-1, *inside)


def two_step_exchange(value, groups, turns, split_dim, concat_dim):
    size = lax.axis_size(groups[0]) * lax.axis_size(groups[1])
    pieces = cut_along(value, split_dim, size)
    return in_order(moved_by_axis(pieces, groups, turns), concat_dim)


def sent_and_summed(value, axis, dim):
    pieces = cut_along(value, dim, lax.axis_size(axis))
    arrived = lax.all_to_all(pieces, axis, split_axis=0, concat_axis=0, tiled=True)
    return arrived.astype(jnp.float32).sum(axis=0)


def in_one_piece(arrays, axis, dim, along):
    both = jnp.concatenate(arrays, axis=along)
    filled, at, done = (sent_and_summed(both, axis, dim), 0, [])
    for a in arrays:
        done.append(lax.slice_in_dim(filled, at, at + a.shape[along], axis=along))
        at += a.shape[along]
    return tuple(done)


def sent_to_all(value, axis):
    size = lax.axis_size(axis)
    return lax.all_to_all(
        jnp.broadcast_to(value[None], (size, *value.shape)), axis, 0, 0, tiled=True
    )


def gathered_copies(value, axis, dim):
    return in_order(sent_to_all(value, axis), dim)


def taken_together(value, axis):
    everything = sent_to_all(value, axis)
    return jnp.sum(everything, axis=0)


def per_device(tokens, expert_ids, gate_weights, w_gate, w_up, w_down):
    expert_count = lax.axis_size(EXPERT)
    hidden_count = lax.axis_size("dp")
    local_experts = w_gate.shape[0]
    tok_rows = tokens.shape[0]
    feature_cols = tokens.shape[1]
    total_experts = local_experts * expert_count
    cap_share = CAP // hidden_count
    flat_ids = expert_ids.reshape(-1)
    one_hot = (flat_ids[:, None] == lax.iota(jnp.int32, total_experts)[None, :]).astype(jnp.int32)
    earlier = jnp.cumsum(one_hot, axis=0) - one_hot
    slot_rank = jnp.sum(earlier * one_hot, axis=1)
    owner_device = flat_ids // local_experts
    within = flat_ids % local_experts
    block_index = lax.axis_index("dp")
    is_mine = slot_rank // cap_share == block_index
    table_cols = local_experts * cap_share * expert_count
    send_slot = (within * cap_share + slot_rank % cap_share) * expert_count + owner_device
    mine_at = jnp.where(is_mine, send_slot, -1)
    dispatch_table = (mine_at[None, :] == lax.iota(jnp.int32, table_cols)[:, None]).astype(
        jnp.float32
    )
    dispatch_table = jnp.sum(dispatch_table.reshape(table_cols, tok_rows, TOP), axis=2).astype(
        jnp.bfloat16
    )
    outbound = jnp.dot(dispatch_table, tokens, preferred_element_type=jnp.float32).astype(
        jnp.bfloat16
    )
    outbound = outbound.reshape(local_experts, cap_share, expert_count, feature_cols)
    arrived = two_step_exchange(outbound, ("expert_0", "expert_1"), (1, 0), 2, 2)
    expert_rows = lax.all_gather(
        arrived.reshape(local_experts, cap_share * expert_count, feature_cols), "dp", axis=1, tiled=True
    )
    gate_part = jnp.einsum("lrd,ldf->lrf", expert_rows, w_gate, preferred_element_type=jnp.float32)
    up_part = jnp.einsum("lrd,ldf->lrf", expert_rows, w_up, preferred_element_type=jnp.float32)
    gate_sum, up_sum = in_one_piece((gate_part, up_part), "tensor", 1, 0)
    hidden_share = (jax.nn.silu(gate_sum) * up_sum).astype(jnp.bfloat16)
    hidden = gathered_copies(hidden_share, "tensor", 1)
    partial_value = jnp.einsum("lrf,lfd->lrd", hidden, w_down, preferred_element_type=jnp.float32)
    outputs = sent_and_summed(partial_value.astype(jnp.bfloat16), "dp", 1)
    backward = outputs.astype(jnp.bfloat16).reshape(local_experts, cap_share, expert_count, feature_cols)
    returned = two_step_exchange(backward, ("expert_0", "expert_1"), (1, 0), 2, 2)
    returned = returned.reshape(table_cols, feature_cols).astype(jnp.float32)
    position = send_slot
    scaled = gate_weights.reshape(-1) * is_mine.astype(jnp.float32)
    combine_table = jnp.where(
        position[:, None] == lax.iota(jnp.int32, table_cols)[None, :], scaled[:, None], 0.0
    )
    combine_table = jnp.sum(combine_table.reshape(tok_rows, TOP, table_cols), axis=1)
    partial_mix = jnp.dot(
        combine_table, returned, precision=lax.Precision.HIGHEST, preferred_element_type=jnp.float32
    )
    mixed = taken_together(partial_mix, "dp")
    return mixed.astype(jnp.bfloat16)


def solution(mesh):
    split = Mesh(
        mesh.devices.reshape(mesh.shape["dp"], 32, 2, mesh.shape["tensor"]),
        ("dp", "expert_0", "expert_1", "tensor"),
    )
    placed = (
        P(EXPERT, "tensor"),
        P(EXPERT, None),
        P(EXPERT, None),
        P(EXPERT, "tensor", "dp"),
        P(EXPERT, "tensor", "dp"),
        P(EXPERT, "dp", "tensor"),
    )
    return jax.shard_map(
        per_device, mesh=split, in_specs=placed, out_specs=P(EXPERT, "tensor"), check_vma=False
    )
```

```python
import jax
import jax.numpy as jnp
from jax import lax
from jax.experimental import pallas as pl
from jax.experimental.pallas import tpu as pltpu
from jax.sharding import PartitionSpec as P

TOP = 8
CAP = 4
NZ = 32
NX = 4
NY = 4
TOK = 24
PADTOK = 32
LANES = 512
EDGE = 64
WINDOW = 4
CHUNKS = 4
HALF = WINDOW * 2 * CAP
ROWS = 2 * HALF
SHARE = ROWS // NX
BASES = (0, 384, 896, 1280)
F32 = jnp.float32
BF16 = jnp.bfloat16


def spread_tree():
    parent = {}
    for o in (4, 8, 12, 16):
        parent[o] = o - 4
    for o in (-4, -8, -12):
        parent[o] = o + 4
    for o in (0, 4, 8, 12):
        parent[o + 1] = o
        parent[o + 2] = o + 1
    for o in (4, 8, 12, 16):
        parent[o - 1] = o
    for o in (0, -4, -8, -12):
        parent[o - 1] = o
        parent[o - 2] = o - 1
    for o in (-4, -8, -12):
        parent[o + 1] = o
    parent[-15] = -14
    return parent


PARENT = spread_tree()
HOP = (1.7, 0.8)
STEP = {"over": 1.5, "gather": 5.0, "sum": 4.5, "hidden": 2.6, "down": 5.0, "back": 18.0}


def plan():
    arrival = {0: 0.0}
    while len(arrival) < NZ:
        for o, p in PARENT.items():
            if o not in arrival and p in arrival:
                arrival[o] = arrival[p] + HOP[0] + HOP[1] * abs(o - p)
    order = sorted(arrival, key=lambda o: (arrival[o], o))
    children = {o: sorted([c for c in PARENT if PARENT[c] == o], key=lambda c: -abs(c - o)) for o in order}
    return arrival, order, children


ARRIVAL, ORDER, CHILDREN = plan()
REACH = sorted({(c - p) % NZ for c, p in PARENT.items()} | {(p - c) % NZ for c, p in PARENT.items()})


def groups_of(i):
    return (i, NZ // WINDOW - 1 - i)


def offsets_of(i):
    return [g * WINDOW + j for g in groups_of(i) for j in range(WINDOW)]


def body(tok_ref, ids_ref, gates_ref, wg_ref, wu_ref, wd_ref, out_ref,
         wg, wu, wd, tv, idv, gav, ga, gb, rows, gu, xin, hid, down, yin, ret, back, table, acc, part, fin,
         lsem, msem, mrem, asem, arem, bsem, brem, ysem, yrem, xsem, xrem, hsem, hrem, dsem, drem, zsem, zrem, psem, fsem, frem):
    e = lax.axis_index("expert")
    x = lax.axis_index("tensor")
    y = lax.axis_index("dp")
    z = e // 2
    c = e % 2
    odd = y % 2
    partner = {"expert": 2 * z + (1 - c)}

    def at_z(off):
        return {"expert": 2 * lax.rem(z + (off % NZ), NZ) + c}

    def at_x(d):
        return {"tensor": lax.rem(x + d, NX)}

    def at_y(d):
        return {"dp": lax.rem(y + d, NY)}

    sent = []

    def remote(src, dst, s, r, to):
        return pltpu.make_async_remote_copy(src_ref=src, dst_ref=dst, send_sem=s, recv_sem=r, device_id=to)

    def send(copy):
        copy.start()
        sent.append(copy)

    pad = jnp.zeros((NZ, PADTOK - TOK, LANES), BF16)
    ga[:, TOK:, :] = pad
    gb[:, TOK:, :] = pad
    barrier = pltpu.get_barrier_semaphore()
    pl.semaphore_signal(barrier, inc=1, device_id=partner)
    for off in REACH:
        pl.semaphore_signal(barrier, inc=1, device_id=at_z(off))
    for d in range(1, NX):
        pl.semaphore_signal(barrier, inc=1, device_id=at_x(d))
    for d in range(1, NY):
        pl.semaphore_signal(barrier, inc=1, device_id=at_y(d))
    base = pl.multiple_of(((7 * y) // 2) * 128, 128)
    loads = [
        pltpu.make_async_copy(tok_ref.at[:, pl.ds(base, LANES)], tv, lsem.at[0]),
        pltpu.make_async_copy(ids_ref, idv.at[0], lsem.at[1]),
        pltpu.make_async_copy(gates_ref, gav.at[0], lsem.at[2]),
        pltpu.make_async_copy(wg_ref, wg, lsem.at[3]),
        pltpu.make_async_copy(wu_ref, wu, lsem.at[4]),
        pltpu.make_async_copy(wd_ref, wd, lsem.at[5]),
    ]
    for copy in loads:
        copy.start()

    def own_lanes(shape):
        lane = lax.broadcasted_iota(jnp.int32, shape, len(shape) - 1)
        return jnp.logical_and(lane >= EDGE * odd, lane < LANES - EDGE + EDGE * odd)

    first_id = (LANES - EDGE) * (1 - odd)
    for copy in loads[:3]:
        copy.wait()
    spot = lax.broadcasted_iota(jnp.int32, (TOP, LANES), 1) == first_id + lax.broadcasted_iota(jnp.int32, (TOP, LANES), 0)
    ids_wide = jnp.dot(idv[0].astype(F32), jnp.where(spot, 1.0, 0.0), precision=lax.Precision.HIGHEST, preferred_element_type=F32)
    ga[0, :TOK, :] = jnp.where(own_lanes((TOK, LANES)), tv[...].astype(F32), ids_wide).astype(BF16)
    pl.semaphore_wait(barrier, 1 + len(REACH) + NX - 1 + NY - 1)

    def block(ref, k):
        return ref.at[k, pl.ds(0, TOK), :]

    def relay(child):
        k = (-PARENT[child]) % NZ
        j = (-child) % NZ
        return remote(block(ga, k), block(ga, j), asem.at[j], arem.at[j], at_z(child - PARENT[child]))

    def over(k):
        return remote(block(ga, k), block(gb, k), bsem.at[k], brem.at[k], partner)

    metas = [
        remote(idv.at[0], idv.at[1], msem.at[0], mrem.at[0], partner),
        remote(gav.at[0], gav.at[1], msem.at[1], mrem.at[1], partner),
    ]

    def pass_on(o):
        k = (-o) % NZ
        if o != 0:
            relay(o).wait_recv()
        for child in CHILDREN[o]:
            send(relay(child))
        send(over(k))
        if o == 0:
            for copy in metas:
                send(copy)

    def make_table():
        for copy in metas:
            copy.wait_recv()
        col = lax.broadcasted_iota(jnp.int32, (2 * TOK, ROWS), 1)
        row = lax.broadcasted_iota(jnp.int32, (2 * TOK, ROWS), 0)
        ids = jnp.concatenate([idv[0], idv[1]], axis=0)
        gates = jnp.concatenate([gav[0], gav[1]], axis=0)
        tri_i = lax.broadcasted_iota(jnp.int32, (2 * TOK, 2 * TOK), 0)
        tri_j = lax.broadcasted_iota(jnp.int32, (2 * TOK, 2 * TOK), 1)
        tri = jnp.where(jnp.logical_and(tri_j < tri_i, tri_i // TOK == tri_j // TOK), 1.0, 0.0).astype(BF16)
        slot = (col % (2 * CAP) - CAP * (row // TOK)).astype(F32)
        for i in range(CHUNKS):
            lo, hi = groups_of(i)
            dz = jnp.where(col < HALF, lo * WINDOW, hi * WINDOW) + (col % HALF) // (2 * CAP)
            wanted = 2 * lax.rem(z + NZ - dz, NZ) + c
            hits = jnp.zeros((2 * TOK, ROWS), F32)
            share = jnp.zeros((2 * TOK, ROWS), F32)
            for k in range(TOP):
                same = ids[:, k:k + 1] == wanted
                hits = hits + jnp.where(same, 1.0, 0.0)
                share = share + jnp.where(same, gates[:, k:k + 1], 0.0)
            rank = jnp.dot(tri, hits.astype(BF16), preferred_element_type=F32)
            table[i] = jnp.where(rank == slot, share, 0.0)

    tok = WINDOW * PADTOK
    lane = lax.broadcasted_iota(jnp.int32, (tok, 128), 1) - EDGE * (1 - odd)
    id_lane = jnp.logical_and(lane >= 0, lane < TOP)
    before_i = lax.broadcasted_iota(jnp.int32, (tok, tok), 0)
    before_j = lax.broadcasted_iota(jnp.int32, (tok, tok), 1)
    before = jnp.where(
        jnp.logical_and(before_i < before_j, before_i // PADTOK == before_j // PADTOK), 1.0, 0.0
    ).astype(BF16)
    slot_of = lax.broadcasted_iota(jnp.int32, (HALF, tok), 0)
    tok_of = lax.broadcasted_iota(jnp.int32, (HALF, tok), 1)
    ones = jnp.ones((HALF, 128), BF16)

    def chosen(held, p):
        ids = jnp.where(odd == 1, held[:, :128].astype(F32), held[:, LANES - 128:].astype(F32))
        named = jnp.where(jnp.logical_and(id_lane, ids == e.astype(F32)), 1.0, 0.0).astype(BF16)
        hit = lax.dot_general(ones, named, (((1,), (1,)), ((), ())), preferred_element_type=F32)
        rank = jnp.dot(hit.astype(BF16), before, preferred_element_type=F32)
        at = ((tok_of // PADTOK) * (2 * CAP) + p * CAP).astype(F32)
        pick = jnp.where(rank + at == slot_of.astype(F32), hit, 0.0).astype(BF16)
        return jnp.dot(pick, held, preferred_element_type=F32)

    def row_copy(i, d):
        return remote(rows.at[y, i], rows.at[y, i], ysem.at[i, d], yrem.at[i, d], at_y(d))

    def select(i):
        for k in offsets_of(i):
            over(k).wait_recv()
        for n, g in enumerate(groups_of(i)):
            own = ga[g * WINDOW:(g + 1) * WINDOW].reshape(tok, LANES)
            other = gb[g * WINDOW:(g + 1) * WINDOW].reshape(tok, LANES)
            picked = chosen(own, 0) + chosen(other, 1)
            rows[y, i, n * HALF:(n + 1) * HALF, :] = jnp.where(own_lanes((HALF, LANES)), picked, 0.0).astype(BF16)
        for d in (2, 1, 3):
            send(row_copy(i, d))

    def sum_copy(i, d):
        return remote(gu.at[i, lax.rem(x + d, NX)], xin.at[i, d - 1], xsem.at[i, d], xrem.at[i, d], at_x(d))

    def multiply(i):
        if i == 0:
            loads[3].wait()
            loads[4].wait()
        for d in (1, 3, 2):
            row_copy(i, d).wait_recv()
        for n, w in ((0, wg), (1, wu)):
            total = jnp.dot(rows[0, i], w[:LANES, :], preferred_element_type=F32)
            for q in range(1, NY):
                total = total + jnp.dot(rows[q, i], w[BASES[q]:BASES[q] + LANES, :], preferred_element_type=F32)
            gu[i, :, :, n * 256:(n + 1) * 256] = total.reshape(NX, SHARE, 256)
        for d in (2, 1, 3):
            send(sum_copy(i, d))

    def hid_copy(i, d):
        return remote(hid.at[i, x], hid.at[i, x], hsem.at[i, d], hrem.at[i, d], at_x(d))

    def activate(i):
        for d in (1, 3, 2):
            sum_copy(i, d).wait_recv()
        sums = (gu[i, x] + xin[i, 0]) + (xin[i, 1] + xin[i, 2])
        gate = sums[:, :256]
        up = sums[:, 256:]
        hid[i, x] = (gate / (1.0 + jnp.exp(-gate)) * up).astype(BF16)
        for d in (2, 1, 3):
            send(hid_copy(i, d))

    def down_copy(i, d):
        return remote(down.at[i, lax.rem(y + d, NY)], yin.at[i, d - 1], dsem.at[i, d], drem.at[i, d], at_y(d))

    def project(i):
        if i == 0:
            loads[5].wait()
        for d in (1, 3, 2):
            hid_copy(i, d).wait_recv()
        hidden = hid[i].reshape(ROWS, 256)
        for q in range(NY):
            down[i, q] = jnp.dot(hidden, wd[:, BASES[q]:BASES[q] + LANES], preferred_element_type=F32).astype(BF16)
        for d in (2, 1, 3):
            send(down_copy(i, d))

    def back_copy(k):
        return remote(ret.at[k], back.at[k], zsem.at[k], zrem.at[k], at_z(k))

    def give_back(i):
        for d in (1, 3, 2):
            down_copy(i, d).wait_recv()
        result = (down[i, y].astype(F32) + yin[i, 0].astype(F32)) + (yin[i, 1].astype(F32) + yin[i, 2].astype(F32))
        result = result.reshape(2, WINDOW, 2 * CAP, LANES).astype(BF16)
        for n, g in enumerate(groups_of(i)):
            ret[g * WINDOW:(g + 1) * WINDOW] = result[n]
        for k in sorted(offsets_of(i), key=lambda k: -min(k, NZ - k)):
            if k == 0:
                back[0] = ret[0]
            else:
                send(back_copy(k))

    def mix(i):
        for k in offsets_of(i):
            if k != 0:
                back_copy(k).wait_recv()
        arrived = jnp.concatenate(
            [back[g * WINDOW:(g + 1) * WINDOW].astype(F32).reshape(HALF, LANES) for g in groups_of(i)], axis=0
        )
        mixed = jnp.dot(table[i], arrived, precision=lax.Precision.HIGHEST, preferred_element_type=F32)
        acc[...] = mixed if i == 0 else acc[...] + mixed

    events = [(ARRIVAL[o], n, pass_on, o) for n, o in enumerate(ORDER)]
    events.append((0.1, 99, lambda _: make_table(), 0))
    for i in range(CHUNKS):
        at = max(ARRIVAL[o] for o in ARRIVAL if (-o) % NZ in offsets_of(i)) + STEP["over"]
        for n, (stage, wait) in enumerate((
            (select, "gather"), (multiply, "sum"), (activate, "hidden"), (project, "down"), (give_back, "back"), (mix, "over"),
        )):
            events.append((at, 100 - n, stage, i))
            at += STEP[wait]
    for _, _, stage, i in sorted(events, key=lambda v: v[:2] + (v[3],)):
        stage(i)

    part[0] = acc[TOK:, :]
    part_copy = remote(part.at[0], part.at[1], psem.at[0], psem.at[1], partner)
    send(part_copy)
    part_copy.wait_recv()
    fin[y] = (acc[:TOK, :] + part[1]).astype(BF16)

    def fin_copy(d):
        return remote(fin.at[y], fin.at[y], fsem.at[d], frem.at[d], at_y(d))

    for d in (2, 1, 3):
        send(fin_copy(d))
    for d in (1, 3, 2):
        fin_copy(d).wait_recv()
    left = lax.broadcasted_iota(jnp.int32, (TOK, 128), 1) < EDGE
    for n in range(2):
        a, b, o = fin[2 * n], fin[2 * n + 1], n * 896
        out_ref[:, o:o + 384] = a[:, :384]
        out_ref[:, o + 384:o + 512] = jnp.where(left, a[:, 384:].astype(F32), b[:, :128].astype(F32)).astype(BF16)
        out_ref[:, o + 512:o + 896] = b[:, 128:]
    for copy in sent:
        copy.wait_send()


def per_device(tokens, expert_ids, gate_weights, w_gate, w_up, w_down):
    dma = pltpu.SemaphoreType.DMA
    vm = pltpu.VMEM
    out = pl.pallas_call(
        body,
        out_shape=jax.ShapeDtypeStruct((TOK, 1792), BF16),
        in_specs=[pl.BlockSpec(memory_space=pl.ANY)] * 6,
        out_specs=pl.BlockSpec(memory_space=pltpu.VMEM),
        scratch_shapes=[
            vm((1792, 256), BF16),
            vm((1792, 256), BF16),
            vm((256, 1792), BF16),
            vm((TOK, LANES), BF16),
            vm((2, TOK, TOP), jnp.int32),
            vm((2, TOK, TOP), F32),
            vm((NZ, PADTOK, LANES), BF16),
            vm((NZ, PADTOK, LANES), BF16),
            vm((NY, CHUNKS, ROWS, LANES), BF16),
            vm((CHUNKS, NX, SHARE, 512), F32),
            vm((CHUNKS, NX - 1, SHARE, 512), F32),
            vm((CHUNKS, NX, SHARE, 256), BF16),
            vm((CHUNKS, NY, ROWS, LANES), BF16),
            vm((CHUNKS, NY - 1, ROWS, LANES), BF16),
            vm((NZ, 2 * CAP, LANES), BF16),
            vm((NZ, 2 * CAP, LANES), BF16),
            vm((CHUNKS, 2 * TOK, ROWS), F32),
            vm((2 * TOK, LANES), F32),
            vm((2, TOK, LANES), F32),
            vm((NY, TOK, LANES), BF16),
            dma((6,)), dma((2,)), dma((2,)),
            dma((NZ,)), dma((NZ,)), dma((NZ,)), dma((NZ,)),
            *[dma((CHUNKS, 4))] * 8,
            dma((NZ,)), dma((NZ,)), dma((2,)), dma((4,)), dma((4,)),
        ],
        compiler_params=pltpu.CompilerParams(
            collective_id=0, has_side_effects=True, vmem_limit_bytes=60 * 1024 * 1024
        ),
    )(tokens, expert_ids, gate_weights, w_gate.reshape(1792, 256), w_up.reshape(1792, 256), w_down.reshape(256, 1792))
    return out


def solution(mesh):
    placed = (
        P("expert", "tensor"),
        P("expert", None),
        P("expert", None),
        P("expert", "tensor", "dp"),
        P("expert", "tensor", "dp"),
        P("expert", "dp", "tensor"),
    )
    return jax.shard_map(
        per_device, mesh=mesh, in_specs=placed, out_specs=P("expert", "tensor"), check_vma=False
    )
```

```python
import jax
import jax.numpy as jnp
from jax import lax
from jax.experimental import pallas as pl
from jax.experimental.pallas import tpu as pltpu
from jax.sharding import PartitionSpec as P

TOP = 8
CAP = 4
NZ = 32
NX = 4
NY = 4
TOK = 24
PADTOK = 32
LANES = 512
EDGE = 64
WINDOW = 2
CHUNKS = 8
HALF = WINDOW * 2 * CAP
ROWS = 2 * HALF
SHARE = ROWS // NX
BASES = (0, 384, 896, 1280)
F32 = jnp.float32
BF16 = jnp.bfloat16


def spread_tree():
    parent = {}
    for o in (4, 8, 12, 16):
        parent[o] = o - 4
    for o in (-4, -8, -12):
        parent[o] = o + 4
    for o in (0, 4, 8, 12):
        parent[o + 1] = o
        parent[o + 2] = o + 1
    for o in (4, 8, 12, 16):
        parent[o - 1] = o
    for o in (0, -4, -8, -12):
        parent[o - 1] = o
        parent[o - 2] = o - 1
    for o in (-4, -8, -12):
        parent[o + 1] = o
    parent[-15] = -14
    return parent


PARENT = spread_tree()
HOP = (2.0, 0.7)
STEP = {"over": 2.5, "gather": 5.2, "sum": 4.8, "hidden": 3.2, "down": 5.2, "back": 18.0}


def plan():
    arrival = {0: 0.0}
    while len(arrival) < NZ:
        for o, p in PARENT.items():
            if o not in arrival and p in arrival:
                arrival[o] = arrival[p] + HOP[0] + HOP[1] * abs(o - p)
    order = sorted(arrival, key=lambda o: (arrival[o], o))
    children = {o: sorted([c for c in PARENT if PARENT[c] == o], key=lambda c: -abs(c - o)) for o in order}
    return arrival, order, children


ARRIVAL, ORDER, CHILDREN = plan()
REACH = sorted({(c - p) % NZ for c, p in PARENT.items()} | {(p - c) % NZ for c, p in PARENT.items()})


def groups_of(i):
    return (i, NZ // WINDOW - 1 - i)


def offsets_of(i):
    return [g * WINDOW + j for g in groups_of(i) for j in range(WINDOW)]


def chunk_of(k):
    return next(i for i in range(CHUNKS) if k in offsets_of(i))


def body(tok_ref, ids_ref, gates_ref, wg_ref, wu_ref, wd_ref, out_ref,
         wg, wu, wd, tv, idv, gav, ga, gb, rows, gu, xin, hid, down, yin, ret, back, table, acc, part, fin, outv,
         lsem, msem, mrem, ssem, arem, brem, yrem, xrem, hrem, drem, zrem, psem, frem):
    e = lax.axis_index("expert")
    x = lax.axis_index("tensor")
    y = lax.axis_index("dp")
    z = e // 2
    c = e % 2
    odd = y % 2
    partner = {"expert": 2 * z + (1 - c)}

    def at_z(off):
        return {"expert": 2 * lax.rem(z + (off % NZ), NZ) + c}

    def at_x(d):
        return {"tensor": lax.rem(x + d, NX)}

    def at_y(d):
        return {"dp": lax.rem(y + d, NY)}

    def turned(a, b):
        return lax.dot_general(
            a, b, (((0,), (0,)), ((), ())), precision=lax.Precision.HIGHEST, preferred_element_type=F32
        )

    def remote(src, dst, s, r, to):
        return pltpu.make_async_remote_copy(src_ref=src, dst_ref=dst, send_sem=s, recv_sem=r, device_id=to)

    def send(copy):
        copy.start()

    def all_of(ref, sem):
        pltpu.make_async_copy(ref, ref, sem).wait()

    pad = jnp.zeros((NZ, PADTOK - TOK, LANES), BF16)
    ga[:, TOK:, :] = pad
    gb[:, TOK:, :] = pad
    barrier = pltpu.get_barrier_semaphore()
    pl.semaphore_signal(barrier, inc=1, device_id=partner)
    for off in REACH:
        pl.semaphore_signal(barrier, inc=1, device_id=at_z(off))
    for d in range(1, NX):
        pl.semaphore_signal(barrier, inc=1, device_id=at_x(d))
    for d in range(1, NY):
        pl.semaphore_signal(barrier, inc=1, device_id=at_y(d))
    base = pl.multiple_of(((7 * y) // 2) * 128, 128)
    loads = [
        pltpu.make_async_copy(tok_ref.at[:, pl.ds(base, LANES)], tv, lsem.at[0]),
        pltpu.make_async_copy(ids_ref, idv.at[0], lsem.at[1]),
        pltpu.make_async_copy(gates_ref, gav.at[0], lsem.at[2]),
        pltpu.make_async_copy(wg_ref, wg, lsem.at[3]),
        pltpu.make_async_copy(wu_ref, wu, lsem.at[4]),
        pltpu.make_async_copy(wd_ref, wd, lsem.at[5]),
    ]
    for copy in loads:
        copy.start()

    def own_lanes(shape):
        lane = lax.broadcasted_iota(jnp.int32, shape, len(shape) - 1)
        return jnp.logical_and(lane >= EDGE * odd, lane < LANES - EDGE + EDGE * odd)

    first_id = (LANES - EDGE) * (1 - odd)
    for copy in loads[:3]:
        copy.wait()
    spot = lax.broadcasted_iota(jnp.int32, (TOP, LANES), 1) == first_id + lax.broadcasted_iota(jnp.int32, (TOP, LANES), 0)
    ids_wide = turned(idv[0].astype(F32), jnp.where(spot, 1.0, 0.0))
    ga[0, :TOK, :] = jnp.where(own_lanes((TOK, LANES)), tv[...].astype(F32), ids_wide).astype(BF16)
    pl.semaphore_wait(barrier, 1 + len(REACH) + NX - 1 + NY - 1)

    def block(ref, k):
        return ref.at[k, pl.ds(0, TOK), :]

    def relay(child):
        k = (-PARENT[child]) % NZ
        j = (-child) % NZ
        return remote(block(ga, k), block(ga, j), ssem.at[0], arem.at[j], at_z(child - PARENT[child]))

    def over(k):
        return remote(block(ga, k), block(gb, k), ssem.at[1], brem.at[chunk_of(k)], partner)

    metas = [
        remote(idv.at[0], idv.at[1], msem.at[0], mrem.at[0], partner),
        remote(gav.at[0], gav.at[1], msem.at[1], mrem.at[1], partner),
    ]

    def pass_on(o):
        k = (-o) % NZ
        if o != 0:
            relay(o).wait_recv()
        for child in CHILDREN[o]:
            send(relay(child))
        send(over(k))
        if o == 0:
            for copy in metas:
                send(copy)

    def make_table():
        for copy in metas:
            copy.wait_recv()
        col = lax.broadcasted_iota(jnp.int32, (2 * TOK, ROWS), 1)
        row = lax.broadcasted_iota(jnp.int32, (2 * TOK, ROWS), 0)
        eye = (lax.broadcasted_iota(jnp.int32, (TOP, 128), 0) == lax.broadcasted_iota(jnp.int32, (TOP, 128), 1)).astype(F32)
        ids = jnp.concatenate([turned(idv[n].astype(F32), eye) for n in range(2)], axis=0)
        gates = jnp.concatenate([turned(gav[n], eye) for n in range(2)], axis=0)
        tri_i = lax.broadcasted_iota(jnp.int32, (2 * TOK, 2 * TOK), 0)
        tri_j = lax.broadcasted_iota(jnp.int32, (2 * TOK, 2 * TOK), 1)
        tri = jnp.where(jnp.logical_and(tri_j < tri_i, tri_i // TOK == tri_j // TOK), 1.0, 0.0).astype(BF16)
        slot = (col % (2 * CAP) - CAP * (row // TOK)).astype(F32)
        for i in range(CHUNKS):
            lo, hi = groups_of(i)
            dz = jnp.where(col < HALF, lo * WINDOW, hi * WINDOW) + (col % HALF) // (2 * CAP)
            wanted = (2 * lax.rem(z + NZ - dz, NZ) + c).astype(F32)
            hits = jnp.zeros((2 * TOK, ROWS), F32)
            share = jnp.zeros((2 * TOK, ROWS), F32)
            for k in range(TOP):
                same = ids[:, k:k + 1] == wanted
                hits = hits + jnp.where(same, 1.0, 0.0)
                share = share + jnp.where(same, gates[:, k:k + 1], 0.0)
            rank = jnp.dot(tri, hits.astype(BF16), preferred_element_type=F32)
            table[i] = jnp.where(rank == slot, share, 0.0)

    part_tok = WINDOW * PADTOK
    tok = 4 * part_tok
    lane = lax.broadcasted_iota(jnp.int32, (tok, 128), 1) - EDGE * (1 - odd)
    id_lane = jnp.logical_and(lane >= 0, lane < TOP)
    before_i = lax.broadcasted_iota(jnp.int32, (tok, tok), 0)
    before_j = lax.broadcasted_iota(jnp.int32, (tok, tok), 1)
    before = jnp.where(
        jnp.logical_and(before_i < before_j, before_i // PADTOK == before_j // PADTOK), 1.0, 0.0
    ).astype(BF16)
    tok_of = lax.broadcasted_iota(jnp.int32, (ROWS, tok), 1)
    slot_of = lax.broadcasted_iota(jnp.int32, (ROWS, tok), 0)
    first_slot = (
        (tok_of // (2 * part_tok)) * HALF
        + ((tok_of % part_tok) // PADTOK) * (2 * CAP)
        + ((tok_of // part_tok) % 2) * CAP
    )
    wanted_rank = (slot_of - first_slot).astype(F32)
    ones = jnp.ones((ROWS, 128), BF16)

    def chosen(held):
        ids = jnp.where(odd == 1, held[:, :128].astype(F32), held[:, LANES - 128:].astype(F32))
        named = jnp.where(jnp.logical_and(id_lane, ids == e.astype(F32)), 1.0, 0.0).astype(BF16)
        hit = lax.dot_general(ones, named, (((1,), (1,)), ((), ())), preferred_element_type=F32)
        rank = jnp.dot(hit.astype(BF16), before, preferred_element_type=F32)
        pick = jnp.where(rank == wanted_rank, hit, 0.0).astype(BF16)
        return jnp.dot(pick, held, preferred_element_type=F32)

    def row_copy(i, d):
        return remote(rows.at[y, i], rows.at[y, i], ssem.at[2], yrem.at[i], at_y(d))

    def select(i):
        all_of(gb.at[pl.ds(0, 2 * WINDOW), pl.ds(0, TOK), :], brem.at[i])
        held = jnp.concatenate(
            [v[g * WINDOW:(g + 1) * WINDOW].reshape(part_tok, LANES) for g in groups_of(i) for v in (ga, gb)], axis=0
        )
        rows[y, i] = jnp.where(own_lanes((ROWS, LANES)), chosen(held), 0.0).astype(BF16)
        for d in (2, 1, 3):
            send(row_copy(i, d))

    def sum_copy(i, d):
        return remote(gu.at[i, lax.rem(x + d, NX)], xin.at[i, d - 1], ssem.at[3], xrem.at[i], at_x(d))

    def multiply(i):
        if i == 0:
            loads[3].wait()
            loads[4].wait()
        all_of(yin.at[i], yrem.at[i])
        for n, w in ((0, wg), (1, wu)):
            total = jnp.dot(rows[0, i], w[:LANES, :], preferred_element_type=F32)
            for q in range(1, NY):
                total = total + jnp.dot(rows[q, i], w[BASES[q]:BASES[q] + LANES, :], preferred_element_type=F32)
            gu[i, :, :, n * 256:(n + 1) * 256] = total.reshape(NX, SHARE, 256)
        for d in (2, 1, 3):
            send(sum_copy(i, d))

    def hid_copy(i, d):
        return remote(hid.at[i, x], hid.at[i, x], ssem.at[4], hrem.at[i], at_x(d))

    def activate(i):
        all_of(xin.at[i], xrem.at[i])
        sums = (gu[i, x] + xin[i, 0]) + (xin[i, 1] + xin[i, 2])
        gate = sums[:, :256]
        up = sums[:, 256:]
        hid[i, x] = (gate / (1.0 + jnp.exp(-gate)) * up).astype(BF16)
        for d in (2, 1, 3):
            send(hid_copy(i, d))

    def down_copy(i, d):
        return remote(down.at[i, lax.rem(y + d, NY)], yin.at[i, d - 1], ssem.at[5], drem.at[i], at_y(d))

    def project(i):
        if i == 0:
            loads[5].wait()
        all_of(hid.at[i, pl.ds(0, NX - 1)], hrem.at[i])
        hidden = hid[i].astype(F32).reshape(ROWS, 256).astype(BF16)
        for q in range(NY):
            down[i, q] = jnp.dot(hidden, wd[:, BASES[q]:BASES[q] + LANES], preferred_element_type=F32).astype(BF16)
        for d in (2, 1, 3):
            send(down_copy(i, d))

    def back_copy(k):
        return remote(ret.at[k], back.at[k], ssem.at[6], zrem.at[chunk_of(k)], at_z(k))

    def give_back(i):
        all_of(yin.at[i], drem.at[i])
        result = (down[i, y].astype(F32) + yin[i, 0].astype(F32)) + (yin[i, 1].astype(F32) + yin[i, 2].astype(F32))
        result = result.reshape(2, WINDOW, 2 * CAP, LANES).astype(BF16)
        for n, g in enumerate(groups_of(i)):
            ret[g * WINDOW:(g + 1) * WINDOW] = result[n]
        for k in sorted(offsets_of(i), key=lambda k: -min(k, NZ - k)):
            if k == 0:
                back[0] = ret[0]
            else:
                send(back_copy(k))

    def mix(i):
        all_of(back.at[pl.ds(0, 2 * WINDOW - (i == 0))], zrem.at[i])
        arrived = jnp.concatenate(
            [back[g * WINDOW:(g + 1) * WINDOW].astype(F32).reshape(HALF, LANES) for g in groups_of(i)], axis=0
        )
        mixed = jnp.dot(table[i], arrived, precision=lax.Precision.HIGHEST, preferred_element_type=F32)
        acc[...] = mixed if i == 0 else acc[...] + mixed

    events = [(ARRIVAL[o], n, pass_on, o) for n, o in enumerate(ORDER)]
    events.append((0.1, 99, lambda _: make_table(), 0))
    for i in range(CHUNKS):
        at = max(ARRIVAL[o] for o in ARRIVAL if (-o) % NZ in offsets_of(i)) + STEP["over"]
        for n, (stage, wait) in enumerate((
            (select, "gather"), (multiply, "sum"), (activate, "hidden"), (project, "down"), (give_back, "back"), (mix, "over"),
        )):
            events.append((at, 100 - n, stage, i))
            at += STEP[wait]
    def settle(n):
        for copy in metas:
            copy.wait_send()
        all_of(ga.at[pl.ds(0, NZ - 1), pl.ds(0, TOK), :], ssem.at[0])
        all_of(gb.at[:, pl.ds(0, TOK), :], ssem.at[1])
        all_of(yin, ssem.at[2])
        all_of(xin, ssem.at[3])
        all_of(hid.at[:, pl.ds(0, NX - 1)], ssem.at[4])
        all_of(yin, ssem.at[5])
        all_of(ret.at[pl.ds(0, NZ - 1)], ssem.at[6])

    late = max(at for at, _, stage, _ in events if stage is give_back)
    events = [v if v[2] is not mix else (max(v[0], late + 1.0), *v[1:]) for v in events]
    events.append((late + 0.5, 0, settle, 0))
    for _, _, stage, i in sorted(events, key=lambda v: v[:2] + (v[3],)):
        stage(i)

    part[0] = acc[TOK:, :]
    part_copy = remote(part.at[0], part.at[1], psem.at[0], psem.at[1], partner)
    send(part_copy)
    part_copy.wait_recv()

    def fin_copy(d):
        return remote(fin.at[y], fin.at[y], ssem.at[7], frem.at[0], at_y(d))

    fin[y] = (acc[:TOK, :] + part[1]).astype(BF16)
    for d in (2, 1, 3):
        send(fin_copy(d))
    all_of(fin.at[pl.ds(0, NY - 1)], frem.at[0])
    left = lax.broadcasted_iota(jnp.int32, (TOK, 128), 1) < EDGE
    for n in range(2):
        a, b, o = fin[2 * n], fin[2 * n + 1], n * 896
        outv[:, o:o + 384] = a[:, :384]
        outv[:, o + 384:o + 512] = jnp.where(left, a[:, 384:].astype(F32), b[:, :128].astype(F32)).astype(BF16)
        outv[:, o + 512:o + 896] = b[:, 128:]
    stored = pltpu.make_async_copy(outv, out_ref, lsem.at[0])
    stored.start()
    part_copy.wait_send()
    all_of(fin.at[pl.ds(0, NY - 1)], ssem.at[7])
    stored.wait()


def per_device(tokens, expert_ids, gate_weights, w_gate, w_up, w_down):
    dma = pltpu.SemaphoreType.DMA
    vm = pltpu.VMEM
    out = pl.pallas_call(
        body,
        out_shape=jax.ShapeDtypeStruct((TOK, 1792), BF16),
        in_specs=[pl.BlockSpec(memory_space=pl.ANY)] * 6,
        out_specs=pl.BlockSpec(memory_space=pl.ANY),
        scratch_shapes=[
            vm((1792, 256), BF16),
            vm((1792, 256), BF16),
            vm((256, 1792), BF16),
            vm((TOK, LANES), BF16),
            vm((2, TOP, TOK), jnp.int32),
            vm((2, TOP, TOK), F32),
            vm((NZ, PADTOK, LANES), BF16),
            vm((NZ, PADTOK, LANES), BF16),
            vm((NY, CHUNKS, ROWS, LANES), BF16),
            vm((CHUNKS, NX, SHARE, 512), F32),
            vm((CHUNKS, NX - 1, SHARE, 512), F32),
            vm((CHUNKS, NX, SHARE, 256), BF16),
            vm((CHUNKS, NY, ROWS, LANES), BF16),
            vm((CHUNKS, NY - 1, ROWS, LANES), BF16),
            vm((NZ, 2 * CAP, LANES), BF16),
            vm((NZ, 2 * CAP, LANES), BF16),
            vm((CHUNKS, 2 * TOK, ROWS), F32),
            vm((2 * TOK, LANES), F32),
            vm((2, TOK, LANES), F32),
            vm((NY, TOK, LANES), BF16),
            vm((TOK, 1792), BF16),
            dma((6,)), dma((2,)), dma((2,)), dma((8,)), dma((NZ,)),
            *[dma((CHUNKS,))] * 6,
            dma((2,)), dma((1,)),
        ],
        compiler_params=pltpu.CompilerParams(
            collective_id=0, has_side_effects=True, vmem_limit_bytes=60 * 1024 * 1024
        ),
    )(tokens, expert_ids.T, gate_weights.T, w_gate.reshape(1792, 256), w_up.reshape(1792, 256), w_down.reshape(256, 1792))
    return out


def solution(mesh):
    placed = (
        P("expert", "tensor"),
        P("expert", None),
        P("expert", None),
        P("expert", "tensor", "dp"),
        P("expert", "tensor", "dp"),
        P("expert", "dp", "tensor"),
    )
    return jax.shard_map(
        per_device, mesh=mesh, in_specs=placed, out_specs=P("expert", "tensor"), check_vma=False
    )
```
